32 devices in a mesh: dp: 8 (over z, x), tensor: 4 (over y, core).
Axes of the slice: x: 2, y: 2, z: 4, core: 2. Of those that a mesh axis runs over, the one named last changes fastest.
Arguments:
- latents: bfloat16 [8, 1056, 1536], P('dp', 'tensor'), may hold values from -6 to 6
- context: bfloat16 [8, 130, 1536], P('dp'), may hold values from -6 to 6
- lengths: int32 [8], P('dp'), may hold values from 769 to 1025, as said below
- cotangent: bfloat16 [8, 1056, 1536], P('dp', 'tensor'), may hold values from -6 to 6
- attn_weights: bfloat16 [8, 1536, 1536], P(None, 'dp', 'tensor')
- mlp_weights: bfloat16 [3, 1536, 6144], P(None, 'dp', 'tensor')
- norm_gains: bfloat16 [3, 1536], P(None, 'dp'), may hold values from 0.5 to 1.5
- attn_momenta: float32 [8, 1536, 1536], P(None, 'dp', 'tensor')
- mlp_momenta: float32 [3, 1536, 6144], P(None, 'dp', 'tensor')
- gain_momenta: float32 [3, 1536], P(None, 'dp'), may hold values from -256 to 256
Outputs:
- output: bfloat16 [8, 1056, 1536], P('dp', 'tensor')
- latent_grad: float32 [8, 1056, 1536], P('dp', 'tensor')
- context_grad: float32 [8, 130, 1536], P('dp', None, 'tensor')
- attn_grad: float32 [8, 1536, 1536], P(None, 'dp', 'tensor')
- mlp_grad: float32 [3, 1536, 6144], P(None, 'dp', 'tensor')
- gain_grad: float32 [3, 1536], P(None, 'dp')
- attn_moment: float32 [8, 1536, 1536], P(None, 'dp', 'tensor')
- mlp_moment: float32 [3, 1536, 6144], P(None, 'dp', 'tensor')
- gain_moment: float32 [3, 1536], P(None, 'dp')
- attn_step: float32 [8, 1536, 1536], P(None, 'dp', 'tensor')
- mlp_step: float32 [3, 1536, 6144], P(None, 'dp', 'tensor')
- gain_step: float32 [3, 1536], P(None, 'dp')
The draws below stay inside these ranges and needn't reach their ends.
Inputs may be any that keep to these rules, and one draw needn't show every extreme that they name: `lengths`: keys at slots at or beyond a sequence's length are ignored; some sequence has exactly 1025.
All inputs are finite; a program needn't handle non-finite values.
Results may differ from the reference program's by a relative error of at most 0.025.
Values may be sent and summed in bfloat16 or wider, within the bound.
A program may use at most 256 MiB of HBM per device.

```python
import math
import jax
import jax.numpy as jnp
from jax import lax

D = 1536
HEADS = 24
HD = 64
FF = 6144
COND = 130
LEN_MAX = 1025
NS_ITERS = 2
SLOTS = 1056
BATCH = 8


def draw_lengths(key, part):
    shortest = LEN_MAX - LEN_MAX // 4
    value_rows = jax.random.randint(key, (BATCH,), shortest, LEN_MAX + 1, dtype=jnp.int32)
    chosen = jax.random.randint(jax.random.fold_in(key, 7), (), 0, BATCH, dtype=jnp.int32)
    return jnp.where(jnp.arange(BATCH, dtype=jnp.int32) == chosen, LEN_MAX, value_rows)


def draw_attn_weights(key, part):
    factors = jnp.array([1.0, 1.0, 1.0, 16.0, 1.0, 1.0, 1.0, 8.0], jnp.float32) * D ** (-0.5)
    value_rows = jax.random.normal(key, (8, D, D), jnp.float32) * factors[:, None, None]
    return value_rows.astype(jnp.bfloat16)


def draw_mlp_weights(key, part):
    factors = jnp.array([D ** (-0.5), D ** (-0.5), FF ** (-0.5)], jnp.float32)
    value_rows = jax.random.normal(key, (3, D, FF), jnp.float32) * factors[:, None, None]
    return value_rows.astype(jnp.bfloat16)


def momentum_values(key, shape):
    rows = jnp.arange(shape[-2], dtype=jnp.float32) / (shape[-2] - 1)
    rising = 1.0 + 2.0 * rows
    magnitude = 0.3 * (BATCH * SLOTS) ** 0.5
    return jax.random.normal(key, shape, jnp.float32) * rising[:, None] * magnitude


def draw_attn_momenta(key, part):
    return momentum_values(jax.random.fold_in(key, 11), (8, D, D))


def draw_mlp_momenta(key, part):
    return momentum_values(jax.random.fold_in(key, 13), (3, D, FF))


def with_spikes(values, key, source, target, parts, factor):
    owner, partner = [(jnp.arange(values.shape[position]) // (values.shape[position] // parts)).reshape([-1 if axis == position else 1 for axis in range(values.ndim)]) for position in (source, target)]
    chosen = jax.random.permutation(key, parts)[partner]
    strong = (owner == chosen) | (owner == (partner + parts // 2) % parts)
    return jnp.where(strong, factor * values, values)


def block_levels(key, shape, pieces, low, high):
    level = 1.0
    for dim, parts in pieces:
        heights = jax.random.uniform(jax.random.fold_in(jax.random.fold_in(key, 6), dim), (parts,), jnp.float32, low / len(pieces), high / len(pieces))
        level = level * jnp.repeat(jnp.exp(heights), shape[dim] // parts).reshape((-1,) + (1,) * (len(shape) - 1 - dim))
    return level


def centred(stream_key, shape, scale, reach, cuts=(), held_as=jnp.bfloat16):
    level = block_levels(stream_key, shape, cuts, -0.22, 0.18) if cuts else 1.0
    values = jax.random.normal(stream_key, shape, jnp.float32) * scale * level
    return jnp.minimum(jnp.maximum(values, -reach), reach).astype(held_as)


def bell_draw_with(key, dims, width, reach, shards, heavy, kind=jnp.bfloat16):
    values = width * jax.random.normal(key, dims, jnp.float32)
    if shards:
        values = values * block_levels(key, dims, shards, -0.22, 0.18)
    return jnp.clip(with_spikes(values, jax.random.fold_in(key, 3), *heavy), -reach, reach).astype(kind)


def setup_inputs(seed: int = 0) -> dict:
    key_list = jax.random.split(jax.random.key(seed), 11)
    latents = bell_draw_with(key_list[0], (BATCH, SLOTS, D), 1.0, 6.0, ((0, 8), (1, 4)), (0, 2, 8, 2.0))
    context = centred(key_list[1], (BATCH, COND, D), 1.0, 6.0, ((0, 8),))
    lengths = draw_lengths(jax.random.fold_in(key_list[10], 71), 0)
    cotangent = bell_draw_with(key_list[3], (BATCH, SLOTS, D), 1.0, 6.0, ((0, 8), (1, 4)), (0, 2, 8, 2.0))
    attn_weights = draw_attn_weights(jax.random.fold_in(key_list[10], 71), 0)
    mlp_weights = draw_mlp_weights(jax.random.fold_in(key_list[10], 71), 0)
    norm_gains = jnp.clip(1.0 + 0.1 * jax.random.normal(key_list[6], (3, D), jnp.float32), 0.5, 1.5).astype(jnp.bfloat16)
    attn_momenta = draw_attn_momenta(jax.random.fold_in(key_list[10], 71), 0)
    mlp_momenta = draw_mlp_momenta(jax.random.fold_in(key_list[10], 71), 0)
    gain_momenta = centred(key_list[9], (3, D), (0.5 * (BATCH * SLOTS) ** 0.5), 256.0, ((1, 8),), jnp.float32)
    return dict(latents=latents, context=context, lengths=lengths, cotangent=cotangent, attn_weights=attn_weights, mlp_weights=mlp_weights, norm_gains=norm_gains, attn_momenta=attn_momenta, mlp_momenta=mlp_momenta, gain_momenta=gain_momenta)


highest = lax.Precision.HIGHEST

@jax.custom_vjp
def low(v):
    return lax.optimization_barrier(v.astype(jnp.bfloat16)).astype(jnp.float32)

@jax.custom_vjp
def low_back(v):
    return v

def low_keep(v):
    return (low(v), None)

def low_pass(kept, grad):
    return (grad,)

def back_keep(v):
    return (v, None)

def back_low(kept, grad):
    return (low(grad),)
low.defvjp(low_keep, low_pass)
low_back.defvjp(back_keep, back_low)

def layer_norm(value_rows, gain):
    center = value_rows - lax.optimization_barrier(jnp.mean(value_rows, axis=-1, keepdims=True))
    spread = lax.optimization_barrier(jnp.mean(center * center, axis=-1, keepdims=True))
    return center * lax.rsqrt(spread + 1e-05) * gain

def rotate(value_rows, direction):
    pair_count = HD // 4
    inverse = jnp.exp(jnp.arange(pair_count, dtype=jnp.float32) * (-math.log(10000.0) / pair_count))
    positions = jnp.arange(value_rows.shape[1], dtype=jnp.float32)
    angles = positions[:, None] * inverse[None, :]
    cosine = jnp.cos(angles)[None, :, None, :]
    sine_part = direction * jnp.sin(angles)[None, :, None, :]
    leading = value_rows[..., :pair_count]
    trailing = value_rows[..., pair_count:2 * pair_count]
    untouched = value_rows[..., 2 * pair_count:]
    return jnp.concatenate([leading * cosine - trailing * sine_part, trailing * cosine + leading * sine_part, untouched], axis=-1)

def project(value_rows, weight_matrix):
    return jnp.einsum('bld,de->ble', value_rows, weight_matrix, precision=highest)

def expand(value_rows, weight_matrix):
    return jnp.einsum('ble,de->bld', value_rows, weight_matrix, precision=highest)

def split_heads(value_rows):
    return value_rows.reshape(value_rows.shape[0], value_rows.shape[1], HEADS, HD)

def merge_heads(value_rows):
    return value_rows.reshape(value_rows.shape[0], value_rows.shape[1], HEADS * HD)

def attend_block(packed):
    query, keys, value, length = packed
    scores = low_back(jnp.einsum('ihd,jhd->hij', query, keys, precision=highest))
    usable = jnp.arange(keys.shape[0], dtype=jnp.int32) < length
    scaled = jnp.where(usable[None, None, :], scores * 0.125, -1000000000.0)
    weights = low(jax.nn.softmax(scaled, axis=-1))
    return jnp.einsum('hij,jhd->ihd', weights, value, precision=highest)

def forward(latents, context, attn_weights, mlp_weights, norm_gains, lengths):
    batch_size = latents.shape[0]
    normed_one = low(layer_norm(latents, norm_gains[0]))
    query_lin = low_back(project(normed_one, attn_weights[0]))
    keys_lin = low_back(project(normed_one, attn_weights[1]))
    value_self = split_heads(low_back(low(project(normed_one, attn_weights[2]))))
    query_self = low(rotate(split_heads(query_lin), 1.0))
    keys_self = low(rotate(split_heads(keys_lin), 1.0))
    attended = lax.map(jax.checkpoint(attend_block), (query_self, keys_self, value_self, lengths))
    attended = low_back(low(merge_heads(attended)))
    resid_one = latents + low_back(expand(attended, attn_weights[3]))
    normed_two = low(layer_norm(resid_one, norm_gains[1]))
    query_cross = split_heads(low_back(low(project(normed_two, attn_weights[4]))))
    keys_cross = split_heads(low_back(low(project(context, attn_weights[5]))))
    value_cross = split_heads(low_back(low(project(context, attn_weights[6]))))
    cond_lengths = jnp.full((batch_size,), COND, jnp.int32)
    crossed = lax.map(jax.checkpoint(attend_block), (query_cross, keys_cross, value_cross, cond_lengths))
    crossed = low_back(low(merge_heads(crossed)))
    resid_two = resid_one + low_back(expand(crossed, attn_weights[7]))
    normed_three = low(layer_norm(resid_two, norm_gains[2]))
    gate = low_back(project(normed_three, mlp_weights[0]))
    upward = low_back(project(normed_three, mlp_weights[1]))
    hidden_state = low(jax.nn.silu(gate) * upward)
    mixed = low_back(jnp.einsum('blf,df->bld', hidden_state, mlp_weights[2], precision=highest))
    return resid_two + mixed

def orthogonalize(moment):
    current = moment / (jnp.sqrt(jnp.sum(moment * moment)) + 1e-07)
    for iteration in range(NS_ITERS):
        gram_matrix = jnp.dot(current, current.T, precision=highest)
        single_term = jnp.dot(gram_matrix, current, precision=highest)
        double_term = jnp.dot(gram_matrix, single_term, precision=highest)
        current = 3.4445 * current - 4.775 * single_term + 2.0315 * double_term
    return current

def reference(latents, context, lengths, cotangent, attn_weights, mlp_weights, norm_gains, attn_momenta, mlp_momenta, gain_momenta):

    def forward_fixed(value_rows, conditioning, attn_w, mlp_w, gain_w):
        return forward(value_rows, conditioning, attn_w, mlp_w, gain_w, lengths)
    result, pull_back = jax.vjp(forward_fixed, latents.astype(jnp.float32), context.astype(jnp.float32), attn_weights.astype(jnp.float32), mlp_weights.astype(jnp.float32), norm_gains.astype(jnp.float32))
    latent_grad, context_grad, attn_grad, mlp_grad, gain_grad = pull_back(cotangent.astype(jnp.float32))
    attn_moment = 0.5 * attn_momenta + 0.5 * attn_grad
    mlp_moment = 0.5 * mlp_momenta + 0.5 * mlp_grad
    gain_moment = 0.5 * gain_momenta + 0.5 * gain_grad
    attn_step = -0.2 * jax.vmap(orthogonalize)(attn_moment)
    mlp_step = -0.2 * max(1.0, FF / D) ** 0.5 * jax.vmap(orthogonalize)(mlp_moment)
    gain_step = -0.001 * gain_moment
    return (result.astype(jnp.bfloat16), latent_grad, context_grad, attn_grad, mlp_grad, gain_grad, attn_moment, mlp_moment, gain_moment, attn_step, mlp_step, gain_step)
```

```python
import functools
import math

import jax
import jax.numpy as jnp
from jax import lax
from jax.experimental import pallas as pl
from jax.experimental.pallas import tpu as pltpu
from jax.sharding import PartitionSpec as P

D = 1536
HD = 64
FF = 6144
NS_ITERS = 2


ns_linear = 3.4445
ns_cubic = -4.775
ns_quintic = 2.0315
muon_rate = 0.2
gain_rate = 0.001
norm_epsilon = 1e-05
muon_epsilon = 1e-07


MESH_ID = pl.DeviceIdType.MESH
CHUNKS = 4
ANY = pl.BlockSpec(memory_space=pl.ANY)
VM = pl.BlockSpec(memory_space=pltpu.VMEM)


def greet(peers):
    barrier = pltpu.get_barrier_semaphore()
    for peer in peers:
        pl.semaphore_signal(barrier, inc=1, device_id=peer, device_id_type=MESH_ID)
    pl.semaphore_wait(barrier, len(peers))


def flip(value, bit):
    if bit == 1:
        return value + 1 - 2 * lax.rem(value, 2)
    return lax.rem(value + 2, 4)


def gather_body(chunks, x_ref, o_ref, send_sem, recv_sem, local_sem):
    d = lax.axis_index("dp")
    t = lax.axis_index("tensor")
    core, chip = flip(t, 1), flip(t, 2)
    width = x_ref.shape[1] // chunks
    greet([(d, core), (d, chip)])
    local = pltpu.make_async_copy(x_ref, o_ref.at[t], local_sem)
    local.start()
    firsts = []
    for j in range(chunks):
        cols = pl.ds(j * width, width)
        firsts.append(
            pltpu.make_async_remote_copy(
                x_ref.at[:, cols], o_ref.at[t, :, cols],
                send_sem.at[j], recv_sem.at[j], device_id=(d, chip), device_id_type=MESH_ID,
            )
        )
        firsts[-1].start()
    side = pltpu.make_async_remote_copy(
        x_ref, o_ref.at[t], send_sem.at[2 * chunks], recv_sem.at[2 * chunks],
        device_id=(d, core), device_id_type=MESH_ID,
    )
    side.start()
    passes = []
    for j in range(chunks):
        cols = pl.ds(j * width, width)
        firsts[j].wait_recv()
        passes.append(
            pltpu.make_async_remote_copy(
                o_ref.at[chip, :, cols], o_ref.at[chip, :, cols],
                send_sem.at[chunks + j], recv_sem.at[chunks + j],
                device_id=(d, core), device_id_type=MESH_ID,
            )
        )
        passes[-1].start()
    for j in range(chunks):
        firsts[j].wait_send()
        passes[j].wait()
    side.wait()
    local.wait()


def tensor_gather(x, cid, chunks=CHUNKS):
    rows, cols = x.shape
    return pl.pallas_call(
        functools.partial(gather_body, chunks),
        out_shape=jax.ShapeDtypeStruct((4, rows, cols), x.dtype),
        in_specs=[VM], out_specs=ANY,
        scratch_shapes=[pltpu.SemaphoreType.DMA((2 * chunks + 1,)),
                        pltpu.SemaphoreType.DMA((2 * chunks + 1,)),
                        pltpu.SemaphoreType.DMA],
        compiler_params=pltpu.CompilerParams(collective_id=cid, has_side_effects=True),
        name=f"tensor_gather_{cid}",
    )(x)


def scatter_body(chunks, p_ref, o_ref, far, own, chipsum, other, far_s, far_r, own_s, own_r, oth_s, oth_r):
    d = lax.axis_index("dp")
    t = lax.axis_index("tensor")
    core, chip = flip(t, 1), flip(t, 2)
    diag = flip(core, 2)
    width = p_ref.shape[2] // chunks
    greet([(d, core), (d, chip)])
    fars, owns, others = [], [], []
    for j in range(chunks):
        cols = pl.ds(j * width, width)
        fars.append(pltpu.make_async_remote_copy(
            p_ref.at[diag, :, cols], far.at[j], far_s.at[j], far_r.at[j],
            device_id=(d, core), device_id_type=MESH_ID))
        fars[-1].start()
    for j in range(chunks):
        cols = pl.ds(j * width, width)
        owns.append(pltpu.make_async_remote_copy(
            p_ref.at[core, :, cols], own.at[j], own_s.at[j], own_r.at[j],
            device_id=(d, core), device_id_type=MESH_ID))
        owns[-1].start()
    for j in range(chunks):
        cols = pl.ds(j * width, width)
        fars[j].wait_recv()
        chipsum[j] = (p_ref[chip, :, cols].astype(jnp.float32) + far[j].astype(jnp.float32)).astype(chipsum.dtype)
        others.append(pltpu.make_async_remote_copy(
            chipsum.at[j], other.at[j], oth_s.at[j], oth_r.at[j],
            device_id=(d, chip), device_id_type=MESH_ID))
        others[-1].start()
    for j in range(chunks):
        cols = pl.ds(j * width, width)
        owns[j].wait_recv()
        others[j].wait_recv()
        o_ref[:, cols] = (p_ref[t, :, cols].astype(jnp.float32) + own[j].astype(jnp.float32)
                          + other[j].astype(jnp.float32)).astype(o_ref.dtype)
    for j in range(chunks):
        fars[j].wait_send()
        owns[j].wait_send()
        others[j].wait_send()


def tensor_scatter(p, cid, out_dtype=jnp.float32, chunks=CHUNKS):
    _, rows, cols = p.shape
    width = cols // chunks
    dma = pltpu.SemaphoreType.DMA((chunks,))
    buf = pltpu.VMEM((chunks, rows, width), p.dtype)
    return pl.pallas_call(
        functools.partial(scatter_body, chunks),
        out_shape=jax.ShapeDtypeStruct((rows, cols), out_dtype),
        in_specs=[VM], out_specs=VM,
        scratch_shapes=[buf, buf, buf, buf, dma, dma, dma, dma, dma, dma],
        compiler_params=pltpu.CompilerParams(collective_id=cid, has_side_effects=True),
        name=f"tensor_scatter_{cid}",
    )(p)


def swap_body(count, x_ref, o_ref, bounce, send_sem, recv_sem, local_sem):
    d = lax.axis_index("dp")
    t = lax.axis_index("tensor")
    greet([(lax.rem(d + k, count), t) for k in range(1, count)])
    copies = []
    for k in range(1, count):
        peer = lax.rem(d + k, count)
        copies.append(pltpu.make_async_remote_copy(
            x_ref.at[peer], o_ref.at[d], send_sem.at[k], recv_sem.at[k],
            device_id=(peer, t), device_id_type=MESH_ID))
        copies[-1].start()
    inward = pltpu.make_async_copy(x_ref.at[d], bounce, local_sem.at[0])
    inward.start()
    inward.wait()
    outward = pltpu.make_async_copy(bounce, o_ref.at[d], local_sem.at[1])
    outward.start()
    for copy in copies:
        copy.wait()
    outward.wait()


def dp_swap(x, cid):
    count, rows, cols = x.shape
    return pl.pallas_call(
        functools.partial(swap_body, count),
        out_shape=jax.ShapeDtypeStruct(x.shape, x.dtype),
        in_specs=[ANY], out_specs=ANY,
        scratch_shapes=[pltpu.VMEM((rows, cols), x.dtype),
                        pltpu.SemaphoreType.DMA((count,)), pltpu.SemaphoreType.DMA((count,)),
                        pltpu.SemaphoreType.DMA((2,))],
        compiler_params=pltpu.CompilerParams(collective_id=cid, has_side_effects=True),
        name=f"dp_swap_{cid}",
    )(x)


ROOTS = (2, 5, 3)


def root_gather_body(count, roots, x_ref, o_ref, bounce, send_sem, recv_sem, local_sem):
    d = lax.axis_index("dp")
    t = lax.axis_index("tensor")
    greet([(lax.rem(d + k, count), t) for k in range(1, count)])
    for step in range(len(roots)):
        for e in range(count):
            m = (e + step) % len(roots)
            root = roots[m]
            if e == root:
                continue
            copy = pltpu.make_async_remote_copy(
                x_ref.at[m], o_ref.at[e], send_sem.at[m], recv_sem.at[e],
                device_id=(root, t), device_id_type=MESH_ID)

            @pl.when(d == e)
            def _():
                copy.start()

    for m, root in enumerate(roots):
        @pl.when(d == root)
        def _():
            inward = pltpu.make_async_copy(x_ref.at[m], bounce, local_sem.at[0])
            inward.start()
            inward.wait()
            outward = pltpu.make_async_copy(bounce, o_ref.at[root], local_sem.at[1])
            outward.start()
            outward.wait()
            for e in range(count):
                if e != root:
                    pltpu.make_async_remote_copy(
                        x_ref.at[m], o_ref.at[e], send_sem.at[m], recv_sem.at[e],
                        device_id=(root, t), device_id_type=MESH_ID).wait_recv()

        @pl.when(d != root)
        def _():
            pltpu.make_async_remote_copy(
                x_ref.at[m], o_ref.at[0], send_sem.at[m], recv_sem.at[0],
                device_id=(root, t), device_id_type=MESH_ID).wait_send()


def root_gather(x, count, cid, roots=ROOTS):
    _, rows, cols = x.shape
    return pl.pallas_call(
        functools.partial(root_gather_body, count, roots),
        out_shape=jax.ShapeDtypeStruct((count, rows, cols), x.dtype),
        in_specs=[ANY], out_specs=ANY,
        scratch_shapes=[pltpu.VMEM((rows, cols), x.dtype),
                        pltpu.SemaphoreType.DMA((len(roots),)), pltpu.SemaphoreType.DMA((count,)),
                        pltpu.SemaphoreType.DMA((2,))],
        compiler_params=pltpu.CompilerParams(collective_id=cid, has_side_effects=True),
        name=f"root_gather_{cid}",
    )(x)


def root_spread_body(count, roots, x_ref, o_ref, bounce, send_sem, recv_sem, local_sem):
    d = lax.axis_index("dp")
    t = lax.axis_index("tensor")
    greet([(lax.rem(d + k, count), t) for k in range(1, count)])
    for m, root in enumerate(roots):
        @pl.when(d == root)
        def _():
            copies = []
            for e in range(count):
                if e != root:
                    copies.append(pltpu.make_async_remote_copy(
                        x_ref.at[e], o_ref.at[m], send_sem.at[e], recv_sem.at[m],
                        device_id=(e, t), device_id_type=MESH_ID))
                    copies[-1].start()
            inward = pltpu.make_async_copy(x_ref.at[root], bounce, local_sem.at[0])
            inward.start()
            inward.wait()
            outward = pltpu.make_async_copy(bounce, o_ref.at[m], local_sem.at[1])
            outward.start()
            outward.wait()
            for copy in copies:
                copy.wait_send()

        @pl.when(d != root)
        def _():
            pltpu.make_async_remote_copy(
                x_ref.at[0], o_ref.at[m], send_sem.at[0], recv_sem.at[m],
                device_id=(root, t), device_id_type=MESH_ID).wait_recv()


def root_spread(x, matrices, cid, roots=ROOTS):
    count, rows, cols = x.shape
    return pl.pallas_call(
        functools.partial(root_spread_body, count, roots),
        out_shape=jax.ShapeDtypeStruct((matrices, rows, cols), x.dtype),
        in_specs=[ANY], out_specs=ANY,
        scratch_shapes=[pltpu.VMEM((rows, cols), x.dtype),
                        pltpu.SemaphoreType.DMA((count,)), pltpu.SemaphoreType.DMA((matrices,)),
                        pltpu.SemaphoreType.DMA((2,))],
        compiler_params=pltpu.CompilerParams(collective_id=cid, has_side_effects=True),
        name=f"root_spread_{cid}",
    )(x)


def layer_norm(value_rows, gain):
    center = value_rows - jnp.mean(value_rows, axis=-1, keepdims=True)
    spread = jnp.mean(center * center, axis=-1, keepdims=True)
    return center * lax.rsqrt(spread + norm_epsilon) * gain


def rotate(value_rows, direction):
    pair_count = HD // 4
    inverse = jnp.exp(jnp.arange(pair_count, dtype=jnp.float32) * (-math.log(10000.0) / pair_count))
    positions = jnp.arange(value_rows.shape[1], dtype=jnp.float32)
    angles = positions[:, None] * inverse[None, :]
    cosine = jnp.cos(angles)[None, :, None, :]
    sine_part = direction * jnp.sin(angles)[None, :, None, :]
    leading = value_rows[..., :pair_count]
    trailing = value_rows[..., pair_count : 2 * pair_count]
    untouched = value_rows[..., 2 * pair_count :]
    return jnp.concatenate(
        [
            leading * cosine - trailing * sine_part,
            trailing * cosine + leading * sine_part,
            untouched,
        ],
        axis=-1,
    )


def attend_forward(query, keys, value, length):
    scores = jnp.einsum("ihd,jhd->hij", query, keys, preferred_element_type=jnp.float32)
    usable = jnp.arange(keys.shape[0], dtype=jnp.int32) < length
    scaled = jnp.where(usable[None, None, :], scores * 0.125, -1000000000.0)
    biggest = jnp.max(scaled, axis=-1, keepdims=True)
    logsum = biggest + jnp.log(jnp.sum(jnp.exp(scaled - biggest), axis=-1, keepdims=True))
    weights = jnp.exp(scaled - logsum).astype(jnp.bfloat16)
    output = jnp.einsum("hij,jhd->ihd", weights, value, preferred_element_type=jnp.float32)
    return (output.astype(jnp.bfloat16), logsum)


def attend_backward(query, keys, value, grad_output, logsum, length):
    scores = jnp.einsum("ihd,jhd->hij", query, keys, preferred_element_type=jnp.float32)
    usable = jnp.arange(keys.shape[0], dtype=jnp.int32) < length
    scaled = jnp.where(usable[None, None, :], scores * 0.125, -1000000000.0)
    probs = jnp.exp(scaled - logsum)
    grad_probs = jnp.einsum("ihd,jhd->hij", grad_output, value, preferred_element_type=jnp.float32)
    grad_value = jnp.einsum(
        "hij,ihd->jhd", probs.astype(jnp.bfloat16), grad_output, preferred_element_type=jnp.float32
    )
    totals = jnp.sum(probs * grad_probs, axis=-1, keepdims=True)
    grad_scores = (probs * (grad_probs - totals) * 0.125).astype(jnp.bfloat16)
    grad_query = jnp.einsum("hij,jhd->ihd", grad_scores, keys, preferred_element_type=jnp.float32)
    grad_keys = jnp.einsum("hij,ihd->jhd", grad_scores, query, preferred_element_type=jnp.float32)
    return (grad_query, grad_keys, grad_value)


def project(value_rows, weight_matrix):
    return jnp.einsum("acz,zy->acy", value_rows, weight_matrix, preferred_element_type=jnp.float32)


def expand(value_rows, weight_matrix):
    return jnp.einsum("xby,ay->xba", value_rows, weight_matrix, preferred_element_type=jnp.float32)


def outer(gradient_tree, value_rows):
    return jnp.einsum("mgf,mgx->xf", gradient_tree, value_rows, preferred_element_type=jnp.float32)

def times(left, right):
    return jnp.dot(left, right, preferred_element_type=jnp.float32)


def half(values):
    return values.astype(jnp.bfloat16)


def inner_product(values):
    return lax.dot_general(values, values, (((1,), (1,)), ((), ())), preferred_element_type=jnp.float32)


def unit_gram(gram):
    size = gram.shape[0]
    rows = lax.broadcasted_iota(jnp.int32, (size, size), 0)
    cols = lax.broadcasted_iota(jnp.int32, (size, size), 1)
    total = jnp.sum(jnp.where(rows == cols, gram.astype(jnp.float32), 0.0))
    scale = 1.0 / (jnp.sqrt(total) + muon_epsilon)
    return half(gram.astype(jnp.float32) * scale * scale), scale


def step_columns(gram, block):
    def poly(values):
        once = times(gram, half(values))
        twice = times(gram, half(once))
        return ns_linear * values + ns_cubic * once + ns_quintic * twice

    first = poly(block.astype(jnp.float32))
    single = poly(poly(times(gram, half(first))))
    double = poly(poly(times(gram, half(single))))
    return ns_linear * first + ns_cubic * single + ns_quintic * double


def step_matrix(gram, block):
    cubic_one = ns_cubic * gram.astype(jnp.float32) + ns_quintic * times(gram, gram)
    low_one = half(cubic_one)
    side = ns_linear * gram.astype(jnp.float32) + times(low_one, gram)
    low_side = half(side)
    gram_two = ns_linear * side + times(low_one, low_side)
    low_two = half(gram_two)
    cubic_two = ns_cubic * gram_two + ns_quintic * times(low_two, low_two)
    rest = ns_linear * (cubic_one + cubic_two) + times(half(cubic_two), low_one)
    return ns_linear * ns_linear * block.astype(jnp.float32) + times(half(rest), block)


def orthogonal_attn(moment):
    count, rows, cols = moment.shape
    block = dp_swap(half(moment), 4).reshape(count * rows, cols)
    whole = tensor_gather(block, 3, 3)
    gram = sum(inner_product(whole[k]) for k in range(4))
    gram, scale = unit_gram(gram)
    result = step_columns(gram, block) * (scale * -muon_rate)
    return dp_swap(half(result).reshape(count, rows, cols), 4).astype(jnp.float32)


def orthogonal_mlp(moment, count):
    matrices, rows, cols = moment.shape
    size = count * rows
    block = root_gather(half(moment), count, 7).reshape(size, cols)
    part = half(inner_product(block))
    gram = tensor_scatter(part.reshape(4, size // 4, size), 5)
    gram = tensor_gather(half(gram), 6).reshape(size, size)
    gram, scale = unit_gram(gram)
    result = step_matrix(gram, block) * (scale * (-muon_rate * max(1.0, FF / D) ** 0.5))
    return root_spread(half(result).reshape(count, rows, cols), matrices, 8).astype(jnp.float32)


def orthogonal_rows(moment, rate):
    total = lax.psum(jnp.sum(moment * moment, axis=(1, 2)), ("dp", "tensor"))
    local = moment / (jnp.sqrt(total) + muon_epsilon)[:, None, None]

    def against(gram, whole):
        return jnp.einsum("mdc,mdr->mcr", gram, whole, preferred_element_type=jnp.float32)

    for iteration in range(NS_ITERS):
        whole = lax.all_gather(half(local), "dp", axis=1, tiled=True)

        def gram_of(values):
            part = jnp.einsum("mdr,mcr->mdc", whole, half(values), preferred_element_type=jnp.float32)
            return half(lax.psum(half(part), "tensor"))

        single = against(gram_of(local), whole)
        double = against(gram_of(single), whole)
        local = ns_linear * local + ns_cubic * single + ns_quintic * double
    return -rate * local


def shards(
    latents,
    context,
    lengths,
    cotangent,
    attn_weights,
    mlp_weights,
    norm_gains,
    attn_momenta,
    mlp_momenta,
    gain_momenta,
):
    seq_count = latents.shape[0]
    inner = attn_weights.shape[2]
    head_local = inner // HD
    dp_count = lax.axis_size("dp")

    def split_heads(value_rows):
        return value_rows.reshape(value_rows.shape[0], value_rows.shape[1], head_local, HD)

    def merge_heads(value_rows):
        return value_rows.reshape(value_rows.shape[0], value_rows.shape[1], inner)

    def spread_rows(value_rows):
        _, rows, cols = value_rows.shape
        return tensor_gather(value_rows[0], 1).reshape(1, 4 * rows, cols)

    def collect_rows(value_rows):
        _, rows, cols = value_rows.shape
        return tensor_scatter(half(value_rows).reshape(4, rows // 4, cols), 2)[None]

    def forward_map(query, keys, value, length_list):
        output, logsum = attend_forward(query[0], keys[0], value[0], length_list[0])
        return output[None], logsum[None]

    def backward_map(query, keys, value, grad_output, logsum, length_list):
        grads = attend_backward(query[0], keys[0], value[0], grad_output[0], logsum[0], length_list[0])
        return tuple(grad[None] for grad in grads)

    def gather_weights(values):
        return lax.all_gather(values, "dp", axis=1, tiled=True)

    def reduce_grads(values):
        return lax.psum_scatter(
            half(jnp.stack(values)), "dp", scatter_dimension=1, tiled=True
        ).astype(jnp.float32)

    gain_values = gather_weights(norm_gains).astype(jnp.float32)
    first_full = gather_weights(attn_weights[:3])
    second_full = gather_weights(attn_weights[3:])
    mlp_full = gather_weights(mlp_weights)
    attn_full = [first_full[k] for k in range(3)] + [second_full[k] for k in range(5)]
    gradient_mixture = spread_rows(cotangent)
    resid_zero = latents.astype(jnp.float32)
    rows_one = spread_rows(half(layer_norm(resid_zero, gain_values[0])))
    query_self = half(rotate(split_heads(project(rows_one, attn_full[0])), 1.0))
    keys_self = half(rotate(split_heads(project(rows_one, attn_full[1])), 1.0))
    value_self = split_heads(half(project(rows_one, attn_full[2])))
    attended, logsum_self = forward_map(query_self, keys_self, value_self, lengths)
    attended = merge_heads(attended)
    resid_one = resid_zero + collect_rows(expand(attended, attn_full[3]))
    rows_two = spread_rows(half(layer_norm(resid_one, gain_values[1])))
    query_cross = split_heads(half(project(rows_two, attn_full[4])))
    keys_cross = split_heads(half(project(context, attn_full[5])))
    value_cross = split_heads(half(project(context, attn_full[6])))
    cond_lengths = jnp.full((seq_count,), keys_cross.shape[1], jnp.int32)
    crossed, logsum_cross = forward_map(query_cross, keys_cross, value_cross, cond_lengths)
    crossed = merge_heads(crossed)
    resid_two = resid_one + collect_rows(expand(crossed, attn_full[7]))
    rows_three = spread_rows(half(layer_norm(resid_two, gain_values[2])))
    gate = project(rows_three, mlp_full[0])
    upward = project(rows_three, mlp_full[1])
    hidden_state = half(jax.nn.silu(gate) * upward)
    grad_hidden = jnp.einsum(
        "zpc,cx->zpx", gradient_mixture, mlp_full[2], preferred_element_type=jnp.float32
    )
    unused_value, gate_pull = jax.vjp(
        lambda gate_in, up_in: jax.nn.silu(gate_in) * up_in, gate, upward
    )
    grad_gate, grad_up = gate_pull(grad_hidden)
    grad_gate = half(grad_gate)
    grad_up = half(grad_up)
    down_weight = jnp.einsum(
        "moj,mor->rj", hidden_state, gradient_mixture, preferred_element_type=jnp.float32
    )
    weight_gate = outer(grad_gate, rows_three)
    weight_up = outer(grad_up, rows_three)
    mlp_grad = reduce_grads([weight_gate, weight_up, down_weight])
    normed_three_grad = collect_rows(
        expand(grad_gate, mlp_full[0]) + expand(grad_up, mlp_full[1])
    )
    unused_norm, norm_pull = jax.vjp(layer_norm, resid_two, gain_values[2])
    resid_grad, gain_three = norm_pull(normed_three_grad)
    grad_two = cotangent.astype(jnp.float32) + resid_grad
    grad_cross_out = spread_rows(half(grad_two))
    result = half(resid_two + collect_rows(expand(hidden_state, mlp_full[2])))
    weight_cross_out = outer(crossed, grad_cross_out)
    grad_crossed = split_heads(half(project(grad_cross_out, attn_full[7])))
    grad_q_cross, grad_k_cross, grad_v_cross = backward_map(
        query_cross, keys_cross, value_cross, grad_crossed, logsum_cross, cond_lengths
    )
    grad_q_cross = merge_heads(half(grad_q_cross))
    grad_k_cross = merge_heads(half(grad_k_cross))
    grad_v_cross = merge_heads(half(grad_v_cross))
    weight_q_cross = outer(grad_q_cross, rows_two)
    weight_k_cross = outer(grad_k_cross, context)
    weight_v_cross = outer(grad_v_cross, context)
    cond_partial = expand(grad_k_cross, attn_full[5]) + expand(grad_v_cross, attn_full[6])
    context_grad = lax.psum_scatter(
        half(cond_partial), "tensor", scatter_dimension=2, tiled=True
    ).astype(jnp.float32)
    normed_two_grad = collect_rows(expand(grad_q_cross, attn_full[4]))
    unused_norm, norm_pull = jax.vjp(layer_norm, resid_one, gain_values[1])
    resid_grad, gain_two = norm_pull(normed_two_grad)
    grad_one = grad_two + resid_grad
    grad_self_out = spread_rows(half(grad_one))
    weight_self_out = outer(attended, grad_self_out)
    late_grad = reduce_grads(
        [weight_self_out, weight_q_cross, weight_k_cross, weight_v_cross, weight_cross_out]
    )
    grad_attended = split_heads(half(project(grad_self_out, attn_full[3])))
    grad_q_self, grad_k_self, grad_v_self = backward_map(
        query_self, keys_self, value_self, grad_attended, logsum_self, lengths
    )
    grad_q_self = merge_heads(half(rotate(grad_q_self, -1.0)))
    grad_k_self = merge_heads(half(rotate(grad_k_self, -1.0)))
    grad_v_self = merge_heads(half(grad_v_self))
    early_grad = reduce_grads(
        [outer(grad_q_self, rows_one), outer(grad_k_self, rows_one), outer(grad_v_self, rows_one)]
    )
    normed_one_grad = collect_rows(
        expand(grad_q_self, attn_full[0])
        + expand(grad_k_self, attn_full[1])
        + expand(grad_v_self, attn_full[2])
    )
    unused_norm, norm_pull = jax.vjp(layer_norm, resid_zero, gain_values[0])
    resid_grad, gain_one = norm_pull(normed_one_grad)
    latent_grad = grad_one + resid_grad
    gain_whole = lax.psum(jnp.stack([gain_one, gain_two, gain_three]), ("dp", "tensor"))
    gain_width = norm_gains.shape[1]
    gain_grad = lax.dynamic_slice_in_dim(gain_whole, lax.axis_index("dp") * gain_width, gain_width, 1)
    attn_grad = jnp.concatenate([early_grad, late_grad])
    attn_moment = 0.5 * attn_momenta + 0.5 * attn_grad
    mlp_moment = 0.5 * mlp_momenta + 0.5 * mlp_grad
    if dp_count == attn_weights.shape[0] and NS_ITERS == 2:
        mlp_step = orthogonal_mlp(mlp_moment, dp_count)
        attn_step = orthogonal_attn(attn_moment)
    else:
        mlp_step = orthogonal_rows(mlp_moment, muon_rate * max(1.0, FF / D) ** 0.5)
        attn_step = orthogonal_rows(attn_moment, muon_rate)
    gain_moment = 0.5 * gain_momenta + 0.5 * gain_grad
    gain_step = -gain_rate * gain_moment
    return (
        result,
        latent_grad,
        context_grad,
        attn_grad,
        mlp_grad,
        gain_grad,
        attn_moment,
        mlp_moment,
        gain_moment,
        attn_step,
        mlp_step,
        gain_step,
    )


def solution(mesh):
    in_specs = (
        P("dp", "tensor", None),
        P("dp", None, None),
        P("dp"),
        P("dp", "tensor", None),
        P(None, "dp", "tensor"),
        P(None, "dp", "tensor"),
        P(None, "dp"),
        P(None, "dp", "tensor"),
        P(None, "dp", "tensor"),
        P(None, "dp"),
    )
    out_specs = (
        P("dp", "tensor", None),
        P("dp", "tensor", None),
        P("dp", None, "tensor"),
        P(None, "dp", "tensor"),
        P(None, "dp", "tensor"),
        P(None, "dp"),
        P(None, "dp", "tensor"),
        P(None, "dp", "tensor"),
        P(None, "dp"),
        P(None, "dp", "tensor"),
        P(None, "dp", "tensor"),
        P(None, "dp"),
    )
    return jax.shard_map(shards, mesh=mesh, in_specs=in_specs, out_specs=out_specs, check_vma=False)
```

```python
import functools
import math

import jax
import jax.numpy as jnp
from jax import lax
from jax.experimental import pallas as pl
from jax.experimental.pallas import tpu as pltpu
from jax.sharding import PartitionSpec as P

D = 1536
HD = 64
FF = 6144
NS_ITERS = 2


ns_linear = 3.4445
ns_cubic = -4.775
ns_quintic = 2.0315
muon_rate = 0.2
gain_rate = 0.001
norm_epsilon = 1e-05
muon_epsilon = 1e-07


MESH_ID = pl.DeviceIdType.MESH
CHUNKS = 4
ANY = pl.BlockSpec(memory_space=pl.ANY)
VM = pl.BlockSpec(memory_space=pltpu.VMEM)


def greet(peers):
    barrier = pltpu.get_barrier_semaphore()
    for peer in peers:
        pl.semaphore_signal(barrier, inc=1, device_id=peer, device_id_type=MESH_ID)
    pl.semaphore_wait(barrier, len(peers))


def flip(value, bit):
    if bit == 1:
        return value + 1 - 2 * lax.rem(value, 2)
    return lax.rem(value + 2, 4)


def gather_body(chunks, x_ref, o_ref, send_sem, recv_sem, local_sem):
    d = lax.axis_index("dp")
    t = lax.axis_index("tensor")
    core, chip = flip(t, 1), flip(t, 2)
    width = x_ref.shape[1] // chunks
    greet([(d, core), (d, chip)])
    local = pltpu.make_async_copy(x_ref, o_ref.at[t], local_sem)
    local.start()
    firsts = []
    for j in range(chunks):
        cols = pl.ds(j * width, width)
        firsts.append(
            pltpu.make_async_remote_copy(
                x_ref.at[:, cols], o_ref.at[t, :, cols],
                send_sem.at[j], recv_sem.at[j], device_id=(d, chip), device_id_type=MESH_ID,
            )
        )
        firsts[-1].start()
    side = pltpu.make_async_remote_copy(
        x_ref, o_ref.at[t], send_sem.at[2 * chunks], recv_sem.at[2 * chunks],
        device_id=(d, core), device_id_type=MESH_ID,
    )
    side.start()
    passes = []
    for j in range(chunks):
        cols = pl.ds(j * width, width)
        firsts[j].wait_recv()
        passes.append(
            pltpu.make_async_remote_copy(
                o_ref.at[chip, :, cols], o_ref.at[chip, :, cols],
                send_sem.at[chunks + j], recv_sem.at[chunks + j],
                device_id=(d, core), device_id_type=MESH_ID,
            )
        )
        passes[-1].start()
    for j in range(chunks):
        firsts[j].wait_send()
        passes[j].wait()
    side.wait()
    local.wait()


def tensor_gather(x, cid, chunks=CHUNKS):
    rows, cols = x.shape
    return pl.pallas_call(
        functools.partial(gather_body, chunks),
        out_shape=jax.ShapeDtypeStruct((4, rows, cols), x.dtype),
        in_specs=[VM], out_specs=ANY,
        scratch_shapes=[pltpu.SemaphoreType.DMA((2 * chunks + 1,)),
                        pltpu.SemaphoreType.DMA((2 * chunks + 1,)),
                        pltpu.SemaphoreType.DMA],
        compiler_params=pltpu.CompilerParams(collective_id=cid, has_side_effects=True),
        cost_estimate=pl.CostEstimate(flops=0, bytes_accessed=75900000, transcendentals=0),
        name=f"tensor_gather_{cid}",
    )(x)


def scatter_body(chunks, p_ref, o_ref, far, own, chipsum, other, far_s, far_r, own_s, own_r, oth_s, oth_r):
    d = lax.axis_index("dp")
    t = lax.axis_index("tensor")
    core, chip = flip(t, 1), flip(t, 2)
    diag = flip(core, 2)
    width = p_ref.shape[2] // chunks
    greet([(d, core), (d, chip)])
    fars, owns, others = [], [], []
    for j in range(chunks):
        cols = pl.ds(j * width, width)
        fars.append(pltpu.make_async_remote_copy(
            p_ref.at[diag, :, cols], far.at[j], far_s.at[j], far_r.at[j],
            device_id=(d, core), device_id_type=MESH_ID))
        fars[-1].start()
    for j in range(chunks):
        cols = pl.ds(j * width, width)
        owns.append(pltpu.make_async_remote_copy(
            p_ref.at[core, :, cols], own.at[j], own_s.at[j], own_r.at[j],
            device_id=(d, core), device_id_type=MESH_ID))
        owns[-1].start()
    for j in range(chunks):
        cols = pl.ds(j * width, width)
        fars[j].wait_recv()
        chipsum[j] = (p_ref[chip, :, cols].astype(jnp.float32) + far[j].astype(jnp.float32)).astype(chipsum.dtype)
        others.append(pltpu.make_async_remote_copy(
            chipsum.at[j], other.at[j], oth_s.at[j], oth_r.at[j],
            device_id=(d, chip), device_id_type=MESH_ID))
        others[-1].start()
    for j in range(chunks):
        cols = pl.ds(j * width, width)
        owns[j].wait_recv()
        others[j].wait_recv()
        o_ref[:, cols] = (p_ref[t, :, cols].astype(jnp.float32) + own[j].astype(jnp.float32)
                          + other[j].astype(jnp.float32)).astype(o_ref.dtype)
    for j in range(chunks):
        fars[j].wait_send()
        owns[j].wait_send()
        others[j].wait_send()


def tensor_scatter(p, cid, out_dtype=jnp.float32, chunks=CHUNKS):
    _, rows, cols = p.shape
    width = cols // chunks
    dma = pltpu.SemaphoreType.DMA((chunks,))
    buf = pltpu.VMEM((chunks, rows, width), p.dtype)
    return pl.pallas_call(
        functools.partial(scatter_body, chunks),
        out_shape=jax.ShapeDtypeStruct((rows, cols), out_dtype),
        in_specs=[VM], out_specs=VM,
        scratch_shapes=[buf, buf, buf, buf, dma, dma, dma, dma, dma, dma],
        compiler_params=pltpu.CompilerParams(collective_id=cid, has_side_effects=True),
        cost_estimate=pl.CostEstimate(flops=0, bytes_accessed=82500000, transcendentals=0),
        name=f"tensor_scatter_{cid}",
    )(p)


def swap_body(count, x_ref, o_ref, bounce, send_sem, recv_sem, local_sem):
    d = lax.axis_index("dp")
    t = lax.axis_index("tensor")
    greet([(lax.rem(d + k, count), t) for k in range(1, count)])
    copies = []
    for k in range(1, count):
        peer = lax.rem(d + k, count)
        copies.append(pltpu.make_async_remote_copy(
            x_ref.at[peer], o_ref.at[d], send_sem.at[k], recv_sem.at[k],
            device_id=(peer, t), device_id_type=MESH_ID))
        copies[-1].start()
    inward = pltpu.make_async_copy(x_ref.at[d], bounce, local_sem.at[0])
    inward.start()
    inward.wait()
    outward = pltpu.make_async_copy(bounce, o_ref.at[d], local_sem.at[1])
    outward.start()
    for copy in copies:
        copy.wait()
    outward.wait()


def dp_swap(x, cid):
    count, rows, cols = x.shape
    return pl.pallas_call(
        functools.partial(swap_body, count),
        out_shape=jax.ShapeDtypeStruct(x.shape, x.dtype),
        in_specs=[ANY], out_specs=ANY,
        scratch_shapes=[pltpu.VMEM((rows, cols), x.dtype),
                        pltpu.SemaphoreType.DMA((count,)), pltpu.SemaphoreType.DMA((count,)),
                        pltpu.SemaphoreType.DMA((2,))],
        compiler_params=pltpu.CompilerParams(collective_id=cid, has_side_effects=True),
        cost_estimate=pl.CostEstimate(flops=0, bytes_accessed=125400000, transcendentals=0),
        name=f"dp_swap_{cid}",
    )(x)


ROOTS = (2, 5, 0)


def small_body(count, x_ref, o_ref, send_sem, recv_sem, local_sem):
    d = lax.axis_index("dp")
    t = lax.axis_index("tensor")
    greet([(lax.rem(d + k, count), t) for k in range(1, count)])
    copies = []
    for k in range(1, count):
        copies.append(pltpu.make_async_remote_copy(
            x_ref, o_ref.at[d], send_sem.at[k], recv_sem.at[k],
            device_id=(lax.rem(d + k, count), t), device_id_type=MESH_ID))
        copies[-1].start()
    local = pltpu.make_async_copy(x_ref, o_ref.at[d], local_sem)
    local.start()
    for copy in copies:
        copy.wait()
    local.wait()


def small_gather(x, count, cid):
    dma = pltpu.SemaphoreType.DMA((count,))
    return pl.pallas_call(
        functools.partial(small_body, count),
        out_shape=jax.ShapeDtypeStruct((count,) + x.shape, x.dtype),
        in_specs=[VM], out_specs=VM,
        scratch_shapes=[dma, dma, pltpu.SemaphoreType.DMA],
        compiler_params=pltpu.CompilerParams(collective_id=cid, has_side_effects=True),
        cost_estimate=pl.CostEstimate(flops=0, bytes_accessed=19800000, transcendentals=0),
        name=f"small_gather_{cid}",
    )(x)


def layer_norm(value_rows, gain):
    center = value_rows - jnp.mean(value_rows, axis=-1, keepdims=True)
    spread = jnp.mean(center * center, axis=-1, keepdims=True)
    return center * lax.rsqrt(spread + norm_epsilon) * gain


def rotate(value_rows, direction):
    pair_count = HD // 4
    inverse = jnp.exp(jnp.arange(pair_count, dtype=jnp.float32) * (-math.log(10000.0) / pair_count))
    positions = jnp.arange(value_rows.shape[1], dtype=jnp.float32)
    angles = positions[:, None] * inverse[None, :]
    cosine = jnp.cos(angles)[None, :, None, :]
    sine_part = direction * jnp.sin(angles)[None, :, None, :]
    leading = value_rows[..., :pair_count]
    trailing = value_rows[..., pair_count : 2 * pair_count]
    untouched = value_rows[..., 2 * pair_count :]
    return jnp.concatenate(
        [
            leading * cosine - trailing * sine_part,
            trailing * cosine + leading * sine_part,
            untouched,
        ],
        axis=-1,
    )


def attend_forward(query, keys, value, length):
    scores = jnp.einsum("ihd,jhd->hij", query, keys, preferred_element_type=jnp.float32)
    usable = jnp.arange(keys.shape[0], dtype=jnp.int32) < length
    scaled = jnp.where(usable[None, None, :], scores * 0.125, -1000000000.0)
    biggest = jnp.max(scaled, axis=-1, keepdims=True)
    logsum = biggest + jnp.log(jnp.sum(jnp.exp(scaled - biggest), axis=-1, keepdims=True))
    weights = jnp.exp(scaled - logsum).astype(jnp.bfloat16)
    output = jnp.einsum("hij,jhd->ihd", weights, value, preferred_element_type=jnp.float32)
    return (output.astype(jnp.bfloat16), logsum)


def attend_backward(query, keys, value, grad_output, logsum, length):
    scores = jnp.einsum("ihd,jhd->hij", query, keys, preferred_element_type=jnp.float32)
    usable = jnp.arange(keys.shape[0], dtype=jnp.int32) < length
    scaled = jnp.where(usable[None, None, :], scores * 0.125, -1000000000.0)
    probs = jnp.exp(scaled - logsum)
    grad_probs = jnp.einsum("ihd,jhd->hij", grad_output, value, preferred_element_type=jnp.float32)
    grad_value = jnp.einsum(
        "hij,ihd->jhd", probs.astype(jnp.bfloat16), grad_output, preferred_element_type=jnp.float32
    )
    totals = jnp.sum(probs * grad_probs, axis=-1, keepdims=True)
    grad_scores = (probs * (grad_probs - totals) * 0.125).astype(jnp.bfloat16)
    grad_query = jnp.einsum("hij,jhd->ihd", grad_scores, keys, preferred_element_type=jnp.float32)
    grad_keys = jnp.einsum("hij,ihd->jhd", grad_scores, query, preferred_element_type=jnp.float32)
    return (grad_query, grad_keys, grad_value)


def project(value_rows, weight_matrix):
    return jnp.einsum("acz,zy->acy", value_rows, weight_matrix, preferred_element_type=jnp.float32)


def expand(value_rows, weight_matrix):
    return jnp.einsum("xby,ay->xba", value_rows, weight_matrix, preferred_element_type=jnp.float32)


def outer(gradient_tree, value_rows):
    return jnp.einsum("mgf,mgx->xf", gradient_tree, value_rows, preferred_element_type=jnp.float32)

def times(left, right):
    return jnp.dot(left, right, preferred_element_type=jnp.float32)


def half(values):
    return values.astype(jnp.bfloat16)


def inner_product(values):
    return lax.dot_general(values, values, (((1,), (1,)), ((), ())), preferred_element_type=jnp.float32)


def diagonal_sum(gram, width=128):
    size = gram.shape[0]
    corners = jnp.stack([gram[k : k + width, k : k + width] for k in range(0, size, width)])
    rows = lax.broadcasted_iota(jnp.int32, corners.shape, 1)
    cols = lax.broadcasted_iota(jnp.int32, corners.shape, 2)
    return jnp.sum(jnp.where(rows == cols, corners.astype(jnp.float32), 0.0))


def unit_gram(gram, total):
    scale = 1.0 / (jnp.sqrt(total) + muon_epsilon)
    return half(gram.astype(jnp.float32) * scale * scale), scale


def step_columns(gram, block):
    def poly(values):
        once = times(gram, half(values))
        twice = times(gram, half(once))
        return ns_linear * values + ns_cubic * once + ns_quintic * twice

    first = poly(block.astype(jnp.float32))
    single = poly(poly(times(gram, half(first))))
    double = poly(poly(times(gram, half(single))))
    return ns_linear * first + ns_cubic * single + ns_quintic * double


def step_matrix(gram, block):
    cubic_one = ns_cubic * gram.astype(jnp.float32) + ns_quintic * times(gram, gram)
    low_one = half(cubic_one)
    side = ns_linear * gram.astype(jnp.float32) + times(low_one, gram)
    low_side = half(side)
    gram_two = ns_linear * side + times(low_one, low_side)
    low_two = half(gram_two)
    cubic_two = ns_cubic * gram_two + ns_quintic * times(low_two, low_two)
    rest = ns_linear * (cubic_one + cubic_two) + times(half(cubic_two), low_one)
    return ns_linear * ns_linear * block.astype(jnp.float32) + times(half(rest), block)


def orthogonal_attn(block, extra, shape):
    size, cols = block.shape
    padded = jnp.pad(half(extra), ((0, 16 - extra.shape[0]), (0, cols - extra.shape[1])))
    whole = tensor_gather(jnp.concatenate([block, padded]), 3, 3)
    summed = jnp.sum(whole[:, size : size + extra.shape[0], : extra.shape[1]].astype(jnp.float32), axis=0)
    whole = whole[:, :size]
    total = jnp.sum(jnp.square(whole.astype(jnp.float32)))
    gram, scale = unit_gram(sum(inner_product(whole[k]) for k in range(4)), total)
    result = step_columns(gram, block) * (scale * -muon_rate)
    return dp_swap(half(result).reshape(shape), 4).astype(jnp.float32), summed


def to_roots(values, roots, count):
    d = lax.axis_index("dp")
    pieces = []
    for k in range(count):
        serves = [((root + k) % count) for root in roots]
        which = sum(m * (d == serves[m]).astype(jnp.int32) for m in range(len(roots)))
        piece = lax.dynamic_index_in_dim(values, which, 0, keepdims=False)
        if k:
            piece = lax.ppermute(piece, "dp", [(serves[m], roots[m]) for m in range(len(roots))])
        pieces.append(piece)
    return jnp.concatenate(pieces)


def from_roots(values, roots, count):
    d = lax.axis_index("dp")
    rows = values.shape[0] // count
    pieces = []
    for k in range(count):
        piece = values[k * rows : (k + 1) * rows]
        if k:
            piece = lax.ppermute(piece, "dp", [(root, (root + k) % count) for root in roots])
        pieces.append(piece)
    stacked = jnp.stack(pieces)
    return jnp.stack(
        [
            lax.dynamic_index_in_dim(stacked, lax.rem(d + count - root, count), 0, keepdims=False)
            for root in roots
        ]
    )


def orthogonal_mlp(block):
    size = block.shape[0]
    part = half(inner_product(block))
    gram = tensor_scatter(part.reshape(4, size // 4, size), 5)
    gram = tensor_gather(half(gram), 6).reshape(size, size)
    gram, scale = unit_gram(gram, diagonal_sum(gram))
    return half(step_matrix(gram, block) * (scale * (-muon_rate * max(1.0, FF / D) ** 0.5)))


def orthogonal_rows(moment, rate):
    total = lax.psum(jnp.sum(moment * moment, axis=(1, 2)), ("dp", "tensor"))
    local = moment / (jnp.sqrt(total) + muon_epsilon)[:, None, None]

    def against(gram, whole):
        return jnp.einsum("mdc,mdr->mcr", gram, whole, preferred_element_type=jnp.float32)

    for iteration in range(NS_ITERS):
        whole = lax.all_gather(half(local), "dp", axis=1, tiled=True)

        def gram_of(values):
            part = jnp.einsum("mdr,mcr->mdc", whole, half(values), preferred_element_type=jnp.float32)
            return half(lax.psum(half(part), "tensor"))

        single = against(gram_of(local), whole)
        double = against(gram_of(single), whole)
        local = ns_linear * local + ns_cubic * single + ns_quintic * double
    return -rate * local


def shards(
    latents,
    context,
    lengths,
    cotangent,
    attn_weights,
    mlp_weights,
    norm_gains,
    attn_momenta,
    mlp_momenta,
    gain_momenta,
):
    seq_count = latents.shape[0]
    inner = attn_weights.shape[2]
    head_local = inner // HD
    dp_count = lax.axis_size("dp")

    def split_heads(value_rows):
        return value_rows.reshape(value_rows.shape[0], value_rows.shape[1], head_local, HD)

    def merge_heads(value_rows):
        return value_rows.reshape(value_rows.shape[0], value_rows.shape[1], inner)

    def spread_rows(value_rows):
        _, rows, cols = value_rows.shape
        return tensor_gather(value_rows[0], 1).reshape(1, 4 * rows, cols)

    def collect_rows(value_rows):
        _, rows, cols = value_rows.shape
        return tensor_scatter(half(value_rows).reshape(4, rows // 4, cols), 2)[None]

    def forward_map(query, keys, value, length_list):
        output, logsum = attend_forward(query[0], keys[0], value[0], length_list[0])
        return output[None], logsum[None]

    def backward_map(query, keys, value, grad_output, logsum, length_list):
        grads = attend_backward(query[0], keys[0], value[0], grad_output[0], logsum[0], length_list[0])
        return tuple(grad[None] for grad in grads)

    def gather_weights(values):
        return lax.all_gather(values, "dp", axis=1, tiled=True)

    def reduce_grads(values):
        return lax.psum_scatter(values, "dp", scatter_dimension=1, tiled=True).astype(jnp.float32)

    attn_full = gather_weights(attn_weights)
    mlp_full = gather_weights(mlp_weights)
    gain_count, gain_width = norm_gains.shape
    padded = jnp.pad(norm_gains, ((0, 16 - gain_count), (0, -gain_width % 128)))
    gain_values = small_gather(padded, dp_count, 9)[:, :gain_count, :gain_width].astype(jnp.float32)
    gain_values = gain_values.transpose(1, 0, 2).reshape(gain_count, dp_count * gain_width)
    gradient_mixture = spread_rows(cotangent)
    resid_zero = latents.astype(jnp.float32)
    rows_one = spread_rows(half(layer_norm(resid_zero, gain_values[0])))
    query_self = half(rotate(split_heads(project(rows_one, attn_full[0])), 1.0))
    keys_self = half(rotate(split_heads(project(rows_one, attn_full[1])), 1.0))
    value_self = split_heads(half(project(rows_one, attn_full[2])))
    attended, logsum_self = forward_map(query_self, keys_self, value_self, lengths)
    attended = merge_heads(attended)
    resid_one = resid_zero + collect_rows(expand(attended, attn_full[3]))
    rows_two = spread_rows(half(layer_norm(resid_one, gain_values[1])))
    query_cross = split_heads(half(project(rows_two, attn_full[4])))
    keys_cross = split_heads(half(project(context, attn_full[5])))
    value_cross = split_heads(half(project(context, attn_full[6])))
    cond_lengths = jnp.full((seq_count,), keys_cross.shape[1], jnp.int32)
    crossed, logsum_cross = forward_map(query_cross, keys_cross, value_cross, cond_lengths)
    crossed = merge_heads(crossed)
    resid_two = resid_one + collect_rows(expand(crossed, attn_full[7]))
    rows_three = spread_rows(half(layer_norm(resid_two, gain_values[2])))
    gate = project(rows_three, mlp_full[0])
    upward = project(rows_three, mlp_full[1])
    hidden_state = half(jax.nn.silu(gate) * upward)
    grad_hidden = jnp.einsum(
        "zpc,cx->zpx", gradient_mixture, mlp_full[2], preferred_element_type=jnp.float32
    )
    unused_value, gate_pull = jax.vjp(
        lambda gate_in, up_in: jax.nn.silu(gate_in) * up_in, gate, upward
    )
    grad_gate, grad_up = gate_pull(grad_hidden)
    grad_gate = half(grad_gate)
    grad_up = half(grad_up)
    down_weight = jnp.einsum(
        "moj,mor->rj", hidden_state, gradient_mixture, preferred_element_type=jnp.float32
    )
    weight_gate = outer(grad_gate, rows_three)
    weight_up = outer(grad_up, rows_three)
    mlp_terms, grad_gate, grad_up, hidden_late = lax.optimization_barrier(
        (half(jnp.stack([weight_gate, weight_up, down_weight])), grad_gate, grad_up, hidden_state)
    )
    mlp_grad = reduce_grads(mlp_terms)
    normed_three_grad = collect_rows(
        expand(grad_gate, mlp_full[0]) + expand(grad_up, mlp_full[1])
    )
    unused_norm, norm_pull = jax.vjp(layer_norm, resid_two, gain_values[2])
    resid_grad, gain_three = norm_pull(normed_three_grad)
    grad_two = cotangent.astype(jnp.float32) + resid_grad
    grad_cross_out = spread_rows(half(grad_two))
    weight_cross_out = outer(crossed, grad_cross_out)
    grad_crossed = split_heads(half(project(grad_cross_out, attn_full[7])))
    grad_q_cross, grad_k_cross, grad_v_cross = backward_map(
        query_cross, keys_cross, value_cross, grad_crossed, logsum_cross, cond_lengths
    )
    grad_q_cross = merge_heads(half(grad_q_cross))
    grad_k_cross = merge_heads(half(grad_k_cross))
    grad_v_cross = merge_heads(half(grad_v_cross))
    weight_q_cross = outer(grad_q_cross, rows_two)
    weight_k_cross = outer(grad_k_cross, context)
    weight_v_cross = outer(grad_v_cross, context)
    cond_partial = expand(grad_k_cross, attn_full[5]) + expand(grad_v_cross, attn_full[6])
    normed_two_grad = collect_rows(expand(grad_q_cross, attn_full[4]))
    unused_norm, norm_pull = jax.vjp(layer_norm, resid_one, gain_values[1])
    resid_grad, gain_two = norm_pull(normed_two_grad)
    grad_one = grad_two + resid_grad
    grad_self_out = spread_rows(half(grad_one))
    weight_self_out = outer(attended, grad_self_out)
    grad_attended = split_heads(half(project(grad_self_out, attn_full[3])))
    grad_q_self, grad_k_self, grad_v_self = backward_map(
        query_self, keys_self, value_self, grad_attended, logsum_self, lengths
    )
    grad_q_self = merge_heads(half(rotate(grad_q_self, -1.0)))
    grad_k_self = merge_heads(half(rotate(grad_k_self, -1.0)))
    grad_v_self = merge_heads(half(grad_v_self))
    fast = dp_count == attn_weights.shape[0] and NS_ITERS == 2
    mlp_moment = 0.5 * mlp_momenta + 0.5 * mlp_grad
    mlp_low, grad_q_self, grad_k_self, grad_v_self = lax.optimization_barrier(
        (half(mlp_moment), grad_q_self, grad_k_self, grad_v_self)
    )
    if fast:
        mlp_block = to_roots(mlp_low, ROOTS, dp_count)
    attn_terms = half(
        jnp.stack(
            [
                outer(grad_q_self, rows_one),
                outer(grad_k_self, rows_one),
                outer(grad_v_self, rows_one),
                weight_self_out,
                weight_q_cross,
                weight_k_cross,
                weight_v_cross,
                weight_cross_out,
            ]
        )
    )
    attn_terms, grad_q_self, grad_k_self, grad_v_self = lax.optimization_barrier(
        (attn_terms, grad_q_self, grad_k_self, grad_v_self)
    )
    attn_grad = reduce_grads(attn_terms)
    normed_one_grad = collect_rows(
        expand(grad_q_self, attn_full[0])
        + expand(grad_k_self, attn_full[1])
        + expand(grad_v_self, attn_full[2])
    )
    unused_norm, norm_pull = jax.vjp(layer_norm, resid_zero, gain_values[0])
    resid_grad, gain_one = norm_pull(normed_one_grad)
    latent_grad = grad_one + resid_grad
    attn_grad, gain_terms, cond_terms = lax.optimization_barrier(
        (attn_grad, half(jnp.stack([gain_one, gain_two, gain_three])), half(cond_partial))
    )
    gain_part = lax.psum_scatter(gain_terms, "dp", scatter_dimension=1, tiled=True)
    context_grad = lax.psum_scatter(
        cond_terms, "tensor", scatter_dimension=2, tiled=True
    ).astype(jnp.float32)
    gain_part, hidden_late = lax.optimization_barrier((gain_part, hidden_late))
    gain_part = gain_part.astype(jnp.float32)
    final_rows = lax.psum_scatter(
        half(expand(hidden_late, mlp_full[2])), "tensor", scatter_dimension=1, tiled=True
    )
    result = half(resid_two + final_rows.astype(jnp.float32))
    attn_moment = 0.5 * attn_momenta + 0.5 * attn_grad
    if fast:
        mlp_rows = orthogonal_mlp(mlp_block)
        mlp_rows, attn_low = lax.optimization_barrier((mlp_rows, half(attn_moment)))
        mlp_step = from_roots(mlp_rows, ROOTS, dp_count).astype(jnp.float32)
        attn_block = dp_swap(attn_low, 4).reshape(-1, inner)
        attn_step, gain_grad = orthogonal_attn(attn_block, gain_part, attn_low.shape)
    else:
        gain_grad = lax.psum(gain_part, "tensor")
        mlp_step = orthogonal_rows(mlp_moment, muon_rate * max(1.0, FF / D) ** 0.5)
        attn_step = orthogonal_rows(attn_moment, muon_rate)
    gain_moment = 0.5 * gain_momenta + 0.5 * gain_grad
    gain_step = -gain_rate * gain_moment
    return (
        result,
        latent_grad,
        context_grad,
        attn_grad,
        mlp_grad,
        gain_grad,
        attn_moment,
        mlp_moment,
        gain_moment,
        attn_step,
        mlp_step,
        gain_step,
    )


def solution(mesh):
    in_specs = (
        P("dp", "tensor", None),
        P("dp", None, None),
        P("dp"),
        P("dp", "tensor", None),
        P(None, "dp", "tensor"),
        P(None, "dp", "tensor"),
        P(None, "dp"),
        P(None, "dp", "tensor"),
        P(None, "dp", "tensor"),
        P(None, "dp"),
    )
    out_specs = (
        P("dp", "tensor", None),
        P("dp", "tensor", None),
        P("dp", None, "tensor"),
        P(None, "dp", "tensor"),
        P(None, "dp", "tensor"),
        P(None, "dp"),
        P(None, "dp", "tensor"),
        P(None, "dp", "tensor"),
        P(None, "dp"),
        P(None, "dp", "tensor"),
        P(None, "dp", "tensor"),
        P(None, "dp"),
    )
    return jax.shard_map(shards, mesh=mesh, in_specs=in_specs, out_specs=out_specs, check_vma=False)
```
